32 devices in a mesh: rep: 2 (over z, core), dp: 16 (over x, y).
Axes of the slice: x: 4, y: 4, z: 1, core: 2. Of those that a mesh axis runs over, the one named last changes fastest.
The devices are a block of a 4x4x8 slice.
Arguments:
- a: bfloat16 [32, 4, 4096, 640], P(('rep', 'dp')), parts along dimension 0
- g: bfloat16 [32, 4, 4096, 3200], P(('rep', 'dp')), parts along dimension 0
Outputs:
- output: bfloat16 [8, 640, 3200], P('rep'), parts along dimension 0
There are 2 independent parts. The reference program is written for one: setup_inputs(seed, part) draws one part's arguments, and reference() takes and returns one part's arrays. A program takes and returns all parts, laid end to end along the dimension named above; each array names one.
All inputs are finite; a program needn't handle non-finite values.
Results may differ from the reference program's by a relative error of at most 0.012.
Values are sent between devices in bfloat16 or wider.
A program may use at most 768 MiB of HBM per device.

```python
import jax
import jax.numpy as jnp
from jax import lax

DEVICES = 16
MATRICES = 4
TOKENS = 4096
D = 640
FF = 3200


def setup_inputs(seed: int = 0, part: int = 0) -> dict:
    ka, kg, ks = (jax.random.fold_in(k, part) for k in jax.random.split(jax.random.key(seed), 3))
    size = 2.0 ** jax.random.uniform(ks, (DEVICES, MATRICES, 1, 1), jnp.float32, -1.0, 1.0)
    a = jax.random.normal(ka, (DEVICES, MATRICES, TOKENS, D), jnp.float32)
    g = size * jax.random.normal(kg, (DEVICES, MATRICES, TOKENS, FF), jnp.float32) * (DEVICES * TOKENS) ** -0.5
    return {"a": a.astype(jnp.bfloat16), "g": g.astype(jnp.bfloat16)}


def reference(a, g):
    def take(so_far, one):
        return so_far + jnp.einsum("ntd,ntf->ndf", *one, preferred_element_type=jnp.float32), None

    return lax.scan(take, jnp.zeros((MATRICES, D, FF), jnp.float32), (a, g))[0].astype(jnp.bfloat16)
```

```python
import functools
import math

import jax
import jax.numpy as jnp
from jax import lax
from jax.experimental import pallas as pl
from jax.experimental.pallas import tpu as pltpu
from jax.sharding import PartitionSpec as P

MESH = pl.DeviceIdType.MESH
LANE = 128
ACC = 6
RING = 8
SENT = 2
BF = jnp.bfloat16
F32 = jnp.float32


def kernel(
    side, a_hbm, g_hbm, out,
    abuf, gbuf, xbuf, acc,
    s0, s1, s2p, s2m, s3,
    r0, r1, r2p, r2m, r3,
    asem, gsem, xsem, send_sem, recv_sem, credit,
):
    mats, tokens, rows = a_hbm.shape
    cols = g_hbm.shape[2]
    chunk = side * LANE
    per = cols // chunk
    whole = mats * per
    total = whole + 1
    half = rows // 2
    band = half // side
    hc = chunk // 2
    up, down = s2p.shape[2], s2m.shape[2]

    me = lax.axis_index("dp")
    ix, iy = me // side, me % side

    def at(x, y):
        return {"dp": lax.rem(x + side, side) * side + lax.rem(y + side, side)}

    near = [[at(ix + 1, iy), at(ix - 1, iy)], [at(ix, iy + 1), at(ix, iy - 1)]]
    pos = [ix, iy]

    def ring(v):
        return lax.rem(v + side, side)

    def load_a(n):
        return pltpu.make_async_copy(a_hbm.at[n], abuf.at[n % 2], asem.at[n % 2])

    def load_g(q):
        n, c = q // per, q % per
        return pltpu.make_async_copy(
            g_hbm.at[n, :, pl.ds(pl.multiple_of(c * chunk, LANE), chunk)], gbuf.at[q % 2], gsem.at[q % 2]
        )

    def load_x(n):
        return pltpu.make_async_copy(g_hbm.at[n, :, pl.ds(per * chunk, LANE)], xbuf, xsem)

    load_a(0).start()
    load_g(0).start()
    load_g(1).start()
    load_x(0).start()

    barrier = pltpu.get_barrier_semaphore()
    for axis in range(2):
        for d in range(2):
            pl.semaphore_signal(barrier, inc=1, device_id=near[axis][d], device_id_type=MESH)
    pl.semaphore_wait(barrier, 4)

    def aslot(q):
        return jnp.where(q == whole, ACC, q % ACC)

    def row0(c, k):
        return pl.multiple_of(c * half + k * band, 16)

    def lane0(l):
        return pl.multiple_of(l * LANE, LANE)

    def piece(q, c, k, l, r0_=0, n=None):
        return out.at[q, pl.ds(row0(c, k) + r0_, band if n is None else n), pl.ds(lane0(l), LANE)]

    def remote(s, q, c, d):
        first, second = c, 1 - c
        p1, p2 = pos[first], pos[second]
        axis = first if s in (0, 1, 6, 7) else second
        w, r = q % SENT, q % RING
        if s == 0:
            src, dst = s0.at[c, d, w], r0.at[c, d, r]
        elif s == 1:
            src, dst = s1.at[c, d, w], r1.at[c, d, r]
        elif s == 2:
            src, dst = (s2p.at[c, w], r2p.at[c, r]) if d == 0 else (s2m.at[c, w], r2m.at[c, r])
        elif s == 3:
            src, dst = s3.at[c, d, w], r3.at[c, d, r]
        elif s == 4:
            src = dst = piece(q, c, p1, p2)
        elif s == 5:
            if d == 0:
                src = dst = piece(q, c, p1, ring(p2 - 1), 0, down)
            else:
                src = dst = piece(q, c, p1, ring(p2 + 1), down, up)
        elif s == 6:
            src = dst = out.at[q, pl.ds(row0(c, p1), band), :]
        else:
            k = ring(p1 - 1) if d == 0 else ring(p1 + 1)
            src = dst = out.at[q, pl.ds(row0(c, k), band), pl.ds(d * hc, hc)]
        return pltpu.make_async_remote_copy(
            src_ref=src, dst_ref=dst,
            send_sem=send_sem.at[s, c, d, w], recv_sem=recv_sem.at[s, c, d, r],
            device_id=near[axis][d], device_id_type=MESH,
        )

    def reuse(s, q, c, d):
        @pl.when(q >= SENT)
        def _():
            remote(s, q, c, d).wait_send()

    def first_sends(q, d):
        slot = aslot(q)
        for c in range(2):
            reuse(0, q, c, d)
            k = ring(pos[c] + 2)
            s0[c, d, q % SENT] = acc[slot, pl.ds(row0(c, k), band), pl.ds(d * hc, hc)].astype(BF)
            remote(0, q, c, d).start()

    def step1(q):
        slot = aslot(q)
        for d in range(2):
            for c in range(2):
                remote(0, q, c, d).wait_recv()
                reuse(1, q, c, d)
                k = ring(pos[c] + (1 if d == 0 else -1))
                r = pl.ds(row0(c, k), band)
                w = q % SENT
                mine, other = pl.ds(d * hc, hc), pl.ds((1 - d) * hc, hc)
                s1[c, d, w, :, mine] = (acc[slot, r, mine] + r0[c, d, q % RING].astype(F32)).astype(BF)
                s1[c, d, w, :, other] = acc[slot, r, other].astype(BF)
                remote(1, q, c, d).start()

    def summed(q, c, l, r0_, n):
        z, lanes = q % RING, pl.ds(lane0(l), LANE)
        v = acc[aslot(q), pl.ds(row0(c, pos[c]) + r0_, n), lanes]
        rs = pl.ds(r0_, n)
        return v + r1[c, 0, z, rs, lanes].astype(F32) + r1[c, 1, z, rs, lanes].astype(F32)

    def step2(q):
        for c in range(2):
            for d in range(2):
                remote(1, q, c, d).wait_recv()
            l = ring(pos[1 - c] + 2)
            w = q % SENT
            for d in range(2):
                reuse(2, q, c, d)
                if d == 0:
                    s2p[c, w] = summed(q, c, l, 0, up).astype(BF)
                else:
                    s2m[c, w] = summed(q, c, l, up, down).astype(BF)
                remote(2, q, c, d).start()

    def step3(q):
        for d in range(2):
            for c in range(2):
                remote(2, q, c, d).wait_recv()
                reuse(3, q, c, d)
                l = ring(pos[1 - c] + (1 if d == 0 else -1))
                w, z = q % SENT, q % RING
                top, low = summed(q, c, l, 0, up), summed(q, c, l, up, down)
                if d == 0:
                    top = top + r2p[c, z].astype(F32)
                else:
                    low = low + r2m[c, z].astype(F32)
                s3[c, d, w, pl.ds(0, up)] = top.astype(BF)
                s3[c, d, w, pl.ds(up, down)] = low.astype(BF)
                remote(3, q, c, d).start()

    def step4(q):
        z = q % RING
        for c in range(2):
            for d in range(2):
                remote(3, q, c, d).wait_recv()
            v = summed(q, c, pos[1 - c], 0, band) + r3[c, 0, z].astype(F32) + r3[c, 1, z].astype(F32)
            out[q, pl.ds(row0(c, pos[c]), band), pl.ds(lane0(pos[1 - c]), LANE)] = v.astype(BF)
            for d in range(2):
                reuse(4, q, c, d)
                remote(4, q, c, d).start()

        @pl.when(q + RING < total)
        def _():
            for axis in range(2):
                for d in range(2):
                    pl.semaphore_signal(
                        credit.at[axis, d], inc=1, device_id=near[axis][d], device_id_type=MESH
                    )

    def arrived(s, q, c, d):
        first, second = c, 1 - c
        p1, p2 = pos[first], pos[second]
        back = -1 if d == 0 else 1
        if s == 4:
            dst = piece(q, c, p1, ring(p2 + back))
        elif s == 5:
            dst = piece(q, c, p1, ring(p2 + 2), 0, down) if d == 0 else piece(q, c, p1, ring(p2 + 2), down, up)
        elif s == 6:
            dst = out.at[q, pl.ds(row0(c, ring(p1 + back)), band), :]
        else:
            dst = out.at[q, pl.ds(row0(c, ring(p1 + 2)), band), pl.ds(d * hc, hc)]
        axis = second if s in (4, 5) else first
        pltpu.make_async_remote_copy(
            src_ref=dst, dst_ref=dst,
            send_sem=send_sem.at[s, c, d, q % SENT], recv_sem=recv_sem.at[s, c, d, q % RING],
            device_id=near[axis][d], device_id_type=MESH,
        ).wait_recv()

    def step5(q):
        for d in range(2):
            for c in range(2):
                arrived(4, q, c, d)
                reuse(5, q, c, d)
                remote(5, q, c, d).start()

    def step6(q):
        for c in range(2):
            for d in range(2):
                arrived(5, q, c, d)
            for d in range(2):
                reuse(6, q, c, d)
                remote(6, q, c, d).start()

    def step7(q):
        for d in range(2):
            for c in range(2):
                arrived(6, q, c, d)
                reuse(7, q, c, d)
                remote(7, q, c, d).start()

    def step8(q):
        for d in range(2):
            for c in range(2):
                arrived(7, q, c, d)

    def dot(n, w):
        return lax.dot_general(abuf[n % 2], w, (((0,), (0,)), ((), ())), preferred_element_type=F32)

    def stage(t, s, f):
        @pl.when((t >= s) & (t < total + s))
        def _():
            f(t - s)

    def turn(t, carry):
        n, c = t // per, t % per

        @pl.when(t < whole)
        def _():
            @pl.when(c == 0)
            def _():
                load_a(n).wait()

                @pl.when(n + 1 < mats)
                def _():
                    load_a(n + 1).start()

            load_g(t).wait()
            acc[t % ACC, :, pl.ds(0, hc)] = dot(n, gbuf[t % 2, :, pl.ds(0, hc)])

        @pl.when((t >= RING) & (t < total))
        def _():
            for axis in range(2):
                for d in range(2):
                    pl.semaphore_wait(credit.at[axis, d], 1)

        @pl.when(t < total)
        def _():
            first_sends(t, 0)

        stage(t, 1, step1)
        stage(t, 2, step2)
        stage(t, 3, step3)
        stage(t, 4, step4)

        @pl.when(t < whole)
        def _():
            acc[t % ACC, :, pl.ds(hc, hc)] = dot(n, gbuf[t % 2, :, pl.ds(hc, hc)])

            @pl.when(t + 2 < whole)
            def _():
                load_g(t + 2).start()

        @pl.when(t < total)
        def _():
            first_sends(t, 1)

        stage(t, 5, step5)
        stage(t, 6, step6)

        @pl.when((t < whole) & (c == per - 1))
        def _():
            load_x(n).wait()
            acc[ACC, :, pl.ds(lane0(n), LANE)] = dot(n, xbuf[...])

            @pl.when(n + 1 < mats)
            def _():
                load_x(n + 1).start()

        stage(t, 7, step7)
        stage(t, 8, step8)
        return carry

    lax.fori_loop(0, total + 8, turn, 0)

    for s in range(8):
        for c in range(2):
            for d in range(2):
                for k in range(SENT):
                    remote(s, total - SENT + k, c, d).wait_send()


def write(per, sums, out, sem):
    mats = out.shape[0]
    chunk = sums.shape[2]
    copies = []
    for n in range(mats):
        for c in range(per):
            copies.append((sums.at[n * per + c], out.at[n, :, pl.ds(c * chunk, chunk)]))
        copies.append((sums.at[mats * per, :, pl.ds(n * LANE, LANE)], out.at[n, :, pl.ds(per * chunk, LANE)]))
    copies = [pltpu.make_async_copy(s, d, sem.at[i]) for i, (s, d) in enumerate(copies)]
    for copy in copies:
        copy.start()
    for copy in copies:
        copy.wait()


def solution(mesh):
    side = math.isqrt(mesh.shape["dp"])

    def step(a, g):
        a, g = a[0], g[0]
        mats, tokens, rows = a.shape
        cols = g.shape[2]
        chunk = side * LANE
        per = cols // chunk
        total = mats * per + 1
        band, hc = rows // 2 // side, chunk // 2
        up = (band // 2 + 15) // 16 * 16
        down = band - up
        dma = pltpu.SemaphoreType.DMA
        sums = pl.pallas_call(
            functools.partial(kernel, side),
            out_shape=pltpu.VMEM((total, rows, chunk), BF),
            in_specs=[pl.BlockSpec(memory_space=pl.ANY)] * 2,
            out_specs=pl.BlockSpec(memory_space=pltpu.VMEM),
            scratch_shapes=[
                pltpu.VMEM((2, tokens, rows), BF),
                pltpu.VMEM((2, tokens, chunk), BF),
                pltpu.VMEM((tokens, LANE), BF),
                pltpu.VMEM((ACC + 1, rows, chunk), F32),
                pltpu.VMEM((2, 2, SENT, band, hc), BF),
                pltpu.VMEM((2, 2, SENT, band, chunk), BF),
                pltpu.VMEM((2, SENT, up, LANE), BF),
                pltpu.VMEM((2, SENT, down, LANE), BF),
                pltpu.VMEM((2, 2, SENT, band, LANE), BF),
                pltpu.VMEM((2, 2, RING, band, hc), BF),
                pltpu.VMEM((2, 2, RING, band, chunk), BF),
                pltpu.VMEM((2, RING, up, LANE), BF),
                pltpu.VMEM((2, RING, down, LANE), BF),
                pltpu.VMEM((2, 2, RING, band, LANE), BF),
                dma((2,)),
                dma((2,)),
                dma(()),
                dma((8, 2, 2, SENT)),
                dma((8, 2, 2, RING)),
                pltpu.SemaphoreType.REGULAR((2, 2)),
            ],
            compiler_params=pltpu.CompilerParams(
                collective_id=0, has_side_effects=True, vmem_limit_bytes=45 * 2**20
            ),
        )(a, g)
        return pl.pallas_call(
            functools.partial(write, per),
            out_shape=jax.ShapeDtypeStruct((mats, rows, cols), BF),
            in_specs=[pl.BlockSpec(memory_space=pltpu.VMEM)],
            out_specs=pl.BlockSpec(memory_space=pl.ANY),
            scratch_shapes=[dma((mats * (per + 1),))],
            compiler_params=pltpu.CompilerParams(vmem_limit_bytes=2**20),
        )(sums)

    return jax.shard_map(
        step,
        mesh=mesh,
        in_specs=(P(("rep", "dp")), P(("rep", "dp"))),
        out_specs=P("rep"),
        check_vma=False,
    )
```

```python
import functools
import math

import jax
import jax.numpy as jnp
from jax import lax
from jax.experimental import pallas as pl
from jax.experimental.pallas import tpu as pltpu
from jax.sharding import PartitionSpec as P

MESH = pl.DeviceIdType.MESH
LANE = 128
ACC = 6
RING = 8
SENT = 2
PARTS = 8
AHEAD = 3
BF = jnp.bfloat16
F32 = jnp.float32


def kernel(
    side, a_hbm, g_hbm, out,
    abuf, gbuf, xbuf, acc,
    s0, s1, s2p, s2m, s3,
    r0, r1, r2p, r2m, r3,
    asem, gsem, xsem, psem, send_sem, recv_sem, credit,
):
    mats, tokens, rows = a_hbm.shape
    cols = g_hbm.shape[2]
    chunk = side * LANE
    per = cols // chunk
    whole = mats * per
    total = whole + 1
    half = rows // 2
    band = half // side
    hc = chunk // 2
    up, down = s2p.shape[2], s2m.shape[2]

    me = lax.axis_index("dp")
    ix, iy = me // side, me % side

    def at(x, y):
        return {"dp": lax.rem(x + side, side) * side + lax.rem(y + side, side)}

    near = [[at(ix + 1, iy), at(ix - 1, iy)], [at(ix, iy + 1), at(ix, iy - 1)]]
    pos = [ix, iy]

    def ring(v):
        return lax.rem(v + side, side)

    def load_a(n):
        return pltpu.make_async_copy(a_hbm.at[n], abuf.at[n % 2], asem.at[n % 2])

    def load_g(q):
        n, c = q // per, q % per
        return pltpu.make_async_copy(
            g_hbm.at[n, :, pl.ds(pl.multiple_of(c * chunk, LANE), chunk)], gbuf.at[q % 2], gsem.at[q % 2]
        )

    def load_x(n):
        return pltpu.make_async_copy(g_hbm.at[n, :, pl.ds(per * chunk, LANE)], xbuf, xsem)

    depth = tokens // PARTS

    def first_loads(k):
        r = pl.ds(pl.multiple_of(k * depth, depth), depth)
        return (
            pltpu.make_async_copy(a_hbm.at[0, r, :], abuf.at[0, r, :], psem.at[0, k]),
            pltpu.make_async_copy(g_hbm.at[0, r, pl.ds(0, chunk)], gbuf.at[0, r, :], psem.at[1, k]),
        )

    for k in range(AHEAD):
        for copy in first_loads(k):
            copy.start()

    barrier = pltpu.get_barrier_semaphore()
    for axis in range(2):
        for d in range(2):
            pl.semaphore_signal(barrier, inc=1, device_id=near[axis][d], device_id_type=MESH)

    acc[0] = jnp.zeros(acc.shape[1:], F32)

    def first_dot(k, carry):
        for copy in first_loads(k):
            copy.wait()

        @pl.when(k + AHEAD < PARTS)
        def _():
            for copy in first_loads(k + AHEAD):
                copy.start()

        @pl.when(k == PARTS - AHEAD)
        def _():
            load_g(1).start()

        r = pl.ds(pl.multiple_of(k * depth, depth), depth)
        for h in range(2):
            lanes = pl.ds(h * hc, hc)
            acc[0, :, lanes] += lax.dot_general(
                abuf[0, r, :], gbuf[0, r, lanes], (((0,), (0,)), ((), ())), preferred_element_type=F32
            )
        return carry

    lax.fori_loop(0, PARTS, first_dot, 0)
    load_a(1).start()
    load_g(2).start()
    load_x(0).start()
    pl.semaphore_wait(barrier, 4)

    def aslot(q):
        return jnp.where(q == whole, ACC, q % ACC)

    def row0(c, k):
        return pl.multiple_of(c * half + k * band, 16)

    def lane0(l):
        return pl.multiple_of(l * LANE, LANE)

    def piece(q, c, k, l, r0_=0, n=None):
        return out.at[q, pl.ds(row0(c, k) + r0_, band if n is None else n), pl.ds(lane0(l), LANE)]

    def remote(s, q, c, d):
        first, second = c, 1 - c
        p1, p2 = pos[first], pos[second]
        axis = first if s in (0, 1, 6, 7) else second
        w, r = q % SENT, q % RING
        if s == 0:
            src, dst = s0.at[c, d, w], r0.at[c, d, r]
        elif s == 1:
            src, dst = s1.at[c, d, w], r1.at[c, d, r]
        elif s == 2:
            src, dst = (s2p.at[c, w], r2p.at[c, r]) if d == 0 else (s2m.at[c, w], r2m.at[c, r])
        elif s == 3:
            src, dst = s3.at[c, d, w], r3.at[c, d, r]
        elif s == 4:
            src = dst = piece(q, c, p1, p2)
        elif s == 5:
            if d == 0:
                src = dst = piece(q, c, p1, ring(p2 - 1), 0, down)
            else:
                src = dst = piece(q, c, p1, ring(p2 + 1), down, up)
        elif s == 6:
            src = dst = out.at[q, pl.ds(row0(c, p1), band), :]
        else:
            k = ring(p1 - 1) if d == 0 else ring(p1 + 1)
            src = dst = out.at[q, pl.ds(row0(c, k), band), pl.ds(d * hc, hc)]
        return pltpu.make_async_remote_copy(
            src_ref=src, dst_ref=dst,
            send_sem=send_sem.at[s, c, d, w], recv_sem=recv_sem.at[s, c, d, r],
            device_id=near[axis][d], device_id_type=MESH,
        )

    def reuse(s, q):
        @pl.when(q >= SENT)
        def _():
            for d in range(2):
                for c in range(2):
                    remote(s, q, c, d).wait_send()

    def step0(q):
        slot = aslot(q)
        reuse(0, q)
        for d in range(2):
            for c in range(2):
                k = ring(pos[c] + 2)
                s0[c, d, q % SENT] = acc[slot, pl.ds(row0(c, k), band), pl.ds(d * hc, hc)].astype(BF)
                remote(0, q, c, d).start()

    def step1(q):
        slot = aslot(q)
        reuse(1, q)
        for d in range(2):
            for c in range(2):
                remote(0, q, c, d).wait_recv()
                k = ring(pos[c] + (1 if d == 0 else -1))
                r = pl.ds(row0(c, k), band)
                w = q % SENT
                mine, other = pl.ds(d * hc, hc), pl.ds((1 - d) * hc, hc)
                s1[c, d, w, :, mine] = (acc[slot, r, mine] + r0[c, d, q % RING].astype(F32)).astype(BF)
                s1[c, d, w, :, other] = acc[slot, r, other].astype(BF)
                remote(1, q, c, d).start()

    def summed(q, c, l, r0_, n):
        z, lanes = q % RING, pl.ds(lane0(l), LANE)
        v = acc[aslot(q), pl.ds(row0(c, pos[c]) + r0_, n), lanes]
        rs = pl.ds(r0_, n)
        return v + r1[c, 0, z, rs, lanes].astype(F32) + r1[c, 1, z, rs, lanes].astype(F32)

    def step2(q):
        reuse(2, q)
        for c in range(2):
            for d in range(2):
                remote(1, q, c, d).wait_recv()
            l = ring(pos[1 - c] + 2)
            w = q % SENT
            for d in range(2):
                if d == 0:
                    s2p[c, w] = summed(q, c, l, 0, up).astype(BF)
                else:
                    s2m[c, w] = summed(q, c, l, up, down).astype(BF)
                remote(2, q, c, d).start()

    def step3(q):
        reuse(3, q)
        for d in range(2):
            for c in range(2):
                remote(2, q, c, d).wait_recv()
                l = ring(pos[1 - c] + (1 if d == 0 else -1))
                w, z = q % SENT, q % RING
                top, low = summed(q, c, l, 0, up), summed(q, c, l, up, down)
                if d == 0:
                    top = top + r2p[c, z].astype(F32)
                else:
                    low = low + r2m[c, z].astype(F32)
                s3[c, d, w, pl.ds(0, up)] = top.astype(BF)
                s3[c, d, w, pl.ds(up, down)] = low.astype(BF)
                remote(3, q, c, d).start()

    def step4(q):
        reuse(4, q)
        z = q % RING
        for c in range(2):
            for d in range(2):
                remote(3, q, c, d).wait_recv()
            v = summed(q, c, pos[1 - c], 0, band) + r3[c, 0, z].astype(F32) + r3[c, 1, z].astype(F32)
            out[q, pl.ds(row0(c, pos[c]), band), pl.ds(lane0(pos[1 - c]), LANE)] = v.astype(BF)
            for d in range(2):
                remote(4, q, c, d).start()

        @pl.when(q + RING < total)
        def _():
            for axis in range(2):
                for d in range(2):
                    pl.semaphore_signal(
                        credit.at[axis, d], inc=1, device_id=near[axis][d], device_id_type=MESH
                    )

    def arrived(s, q, c, d):
        first, second = c, 1 - c
        p1, p2 = pos[first], pos[second]
        back = -1 if d == 0 else 1
        if s == 4:
            dst = piece(q, c, p1, ring(p2 + back))
        elif s == 5:
            dst = piece(q, c, p1, ring(p2 + 2), 0, down) if d == 0 else piece(q, c, p1, ring(p2 + 2), down, up)
        elif s == 6:
            dst = out.at[q, pl.ds(row0(c, ring(p1 + back)), band), :]
        else:
            dst = out.at[q, pl.ds(row0(c, ring(p1 + 2)), band), pl.ds(d * hc, hc)]
        axis = second if s in (4, 5) else first
        pltpu.make_async_remote_copy(
            src_ref=dst, dst_ref=dst,
            send_sem=send_sem.at[s, c, d, q % SENT], recv_sem=recv_sem.at[s, c, d, q % RING],
            device_id=near[axis][d], device_id_type=MESH,
        ).wait_recv()

    def step5(q):
        reuse(5, q)
        for d in range(2):
            for c in range(2):
                arrived(4, q, c, d)
                remote(5, q, c, d).start()

    def step6(q):
        reuse(6, q)
        for c in range(2):
            for d in range(2):
                arrived(5, q, c, d)
            for d in range(2):
                remote(6, q, c, d).start()

    def step7(q):
        reuse(7, q)
        for d in range(2):
            for c in range(2):
                arrived(6, q, c, d)
                remote(7, q, c, d).start()

    def step8(q):
        for d in range(2):
            for c in range(2):
                arrived(7, q, c, d)

    def dot(n, w):
        return lax.dot_general(abuf[n % 2], w, (((0,), (0,)), ((), ())), preferred_element_type=F32)

    def stage(t, s, f):
        @pl.when((t >= s) & (t < total + s))
        def _():
            f(t - s)

    def turn(t, carry):
        u = t + 1
        n, c = u // per, u % per

        @pl.when((t >= RING) & (t < total))
        def _():
            for axis in range(2):
                for d in range(2):
                    pl.semaphore_wait(credit.at[axis, d], 1)

        stage(t, 0, step0)
        stage(t, 1, step1)

        @pl.when(u < whole)
        def _():
            @pl.when(c == 0)
            def _():
                load_a(n).wait()

            load_g(u).wait()
            acc[u % ACC, :, pl.ds(0, hc)] = dot(n, gbuf[u % 2, :, pl.ds(0, hc)])

        stage(t, 2, step2)
        stage(t, 3, step3)
        stage(t, 4, step4)

        @pl.when(u < whole)
        def _():
            acc[u % ACC, :, pl.ds(hc, hc)] = dot(n, gbuf[u % 2, :, pl.ds(hc, hc)])

            @pl.when(u + 2 < whole)
            def _():
                load_g(u + 2).start()

        stage(t, 5, step5)
        stage(t, 6, step6)

        @pl.when((c == 0) & (u <= whole))
        def _():
            load_x(n - 1).wait()
            acc[ACC, :, pl.ds(lane0(n - 1), LANE)] = dot(n - 1, xbuf[...])

            @pl.when(n < mats)
            def _():
                load_x(n).start()

            @pl.when(n + 1 < mats)
            def _():
                load_a(n + 1).start()

        stage(t, 7, step7)
        stage(t, 8, step8)
        return carry

    lax.fori_loop(0, total + 8, turn, 0)

    for s in range(8):
        for c in range(2):
            for d in range(2):
                for k in range(SENT):
                    remote(s, total - SENT + k, c, d).wait_send()


def write(per, sums, out, sem):
    mats = out.shape[0]
    chunk = sums.shape[2]
    copies = []
    for n in range(mats):
        for c in range(per):
            copies.append((sums.at[n * per + c], out.at[n, :, pl.ds(c * chunk, chunk)]))
        copies.append((sums.at[mats * per, :, pl.ds(n * LANE, LANE)], out.at[n, :, pl.ds(per * chunk, LANE)]))
    copies = [pltpu.make_async_copy(s, d, sem.at[i]) for i, (s, d) in enumerate(copies)]
    for copy in copies:
        copy.start()
    for copy in copies:
        copy.wait()


def solution(mesh):
    side = math.isqrt(mesh.shape["dp"])

    def step(a, g):
        a, g = a[0], g[0]
        mats, tokens, rows = a.shape
        cols = g.shape[2]
        chunk = side * LANE
        per = cols // chunk
        total = mats * per + 1
        band, hc = rows // 2 // side, chunk // 2
        up = (band // 2 + 15) // 16 * 16
        down = band - up
        dma = pltpu.SemaphoreType.DMA
        sums = pl.pallas_call(
            functools.partial(kernel, side),
            out_shape=pltpu.VMEM((total, rows, chunk), BF),
            in_specs=[pl.BlockSpec(memory_space=pl.ANY)] * 2,
            out_specs=pl.BlockSpec(memory_space=pltpu.VMEM),
            scratch_shapes=[
                pltpu.VMEM((2, tokens, rows), BF),
                pltpu.VMEM((2, tokens, chunk), BF),
                pltpu.VMEM((tokens, LANE), BF),
                pltpu.VMEM((ACC + 1, rows, chunk), F32),
                pltpu.VMEM((2, 2, SENT, band, hc), BF),
                pltpu.VMEM((2, 2, SENT, band, chunk), BF),
                pltpu.VMEM((2, SENT, up, LANE), BF),
                pltpu.VMEM((2, SENT, down, LANE), BF),
                pltpu.VMEM((2, 2, SENT, band, LANE), BF),
                pltpu.VMEM((2, 2, RING, band, hc), BF),
                pltpu.VMEM((2, 2, RING, band, chunk), BF),
                pltpu.VMEM((2, RING, up, LANE), BF),
                pltpu.VMEM((2, RING, down, LANE), BF),
                pltpu.VMEM((2, 2, RING, band, LANE), BF),
                dma((2,)),
                dma((2,)),
                dma(()),
                dma((2, PARTS)),
                dma((8, 2, 2, SENT)),
                dma((8, 2, 2, RING)),
                pltpu.SemaphoreType.REGULAR((2, 2)),
            ],
            compiler_params=pltpu.CompilerParams(
                collective_id=0, has_side_effects=True, vmem_limit_bytes=45 * 2**20
            ),
        )(a, g)
        return pl.pallas_call(
            functools.partial(write, per),
            out_shape=jax.ShapeDtypeStruct((mats, rows, cols), BF),
            in_specs=[pl.BlockSpec(memory_space=pltpu.VMEM)],
            out_specs=pl.BlockSpec(memory_space=pl.ANY),
            scratch_shapes=[dma((mats * (per + 1),))],
            compiler_params=pltpu.CompilerParams(vmem_limit_bytes=2**20),
        )(sums)

    return jax.shard_map(
        step,
        mesh=mesh,
        in_specs=(P(("rep", "dp")), P(("rep", "dp"))),
        out_specs=P("rep"),
        check_vma=False,
    )
```

```python
import functools
import math

import jax
import jax.numpy as jnp
from jax import lax
from jax.experimental import pallas as pl
from jax.experimental.pallas import tpu as pltpu
from jax.sharding import PartitionSpec as P

MESH = pl.DeviceIdType.MESH
LANE = 128
ACC = 6
RING = 8
SENT = 2
PARTS = 8
AHEAD = 3
ORDER = (0, 1, 'D', 2, 3, 4, 5, 'X', 7, 6, 'D', 8)
LAG = (0, 1, 2, 3, 4, 5, 6, 8, 9)
BF = jnp.bfloat16
F32 = jnp.float32


def kernel(
    side, a_hbm, g_hbm, out,
    abuf, gbuf, xbuf, acc,
    s0, s1, s2p, s2m, s3,
    r0, r1, r2p, r2m, r3,
    asem, gsem, xsem, psem, send_sem, recv_sem, credit,
):
    mats, tokens, rows = a_hbm.shape
    cols = g_hbm.shape[2]
    chunk = side * LANE
    per = cols // chunk
    whole = mats * per
    total = whole + 1
    half = rows // 2
    band = half // side
    hc = chunk // 2
    up, down = s2p.shape[2], s2m.shape[2]

    me = lax.axis_index("dp")
    ix, iy = me // side, me % side

    def at(x, y):
        return {"dp": lax.rem(x + side, side) * side + lax.rem(y + side, side)}

    near = [[at(ix + 1, iy), at(ix - 1, iy)], [at(ix, iy + 1), at(ix, iy - 1)]]
    pos = [ix, iy]

    def ring(v):
        return lax.rem(v + side, side)

    def load_a(n):
        return pltpu.make_async_copy(a_hbm.at[n], abuf.at[n % 2], asem.at[n % 2])

    def load_g(q):
        n, c = q // per, q % per
        return pltpu.make_async_copy(
            g_hbm.at[n, :, pl.ds(pl.multiple_of(c * chunk, LANE), chunk)], gbuf.at[q % 2], gsem.at[q % 2]
        )

    def load_x(n):
        return pltpu.make_async_copy(g_hbm.at[n, :, pl.ds(per * chunk, LANE)], xbuf, xsem)

    depth = tokens // PARTS

    def first_loads(k):
        r = pl.ds(pl.multiple_of(k * depth, depth), depth)
        return (
            pltpu.make_async_copy(a_hbm.at[0, r, :], abuf.at[0, r, :], psem.at[0, k]),
            pltpu.make_async_copy(g_hbm.at[0, r, pl.ds(0, chunk)], gbuf.at[0, r, :], psem.at[1, k]),
        )

    for k in range(AHEAD):
        for copy in first_loads(k):
            copy.start()

    barrier = pltpu.get_barrier_semaphore()
    for axis in range(2):
        for d in range(2):
            pl.semaphore_signal(barrier, inc=1, device_id=near[axis][d], device_id_type=MESH)

    acc[0] = jnp.zeros(acc.shape[1:], F32)

    def first_dot(k, carry):
        for copy in first_loads(k):
            copy.wait()

        @pl.when(k + AHEAD < PARTS)
        def _():
            for copy in first_loads(k + AHEAD):
                copy.start()

        @pl.when(k == PARTS - AHEAD)
        def _():
            load_g(1).start()

        r = pl.ds(pl.multiple_of(k * depth, depth), depth)
        for h in range(2):
            lanes = pl.ds(h * hc, hc)
            acc[0, :, lanes] += lax.dot_general(
                abuf[0, r, :], gbuf[0, r, lanes], (((0,), (0,)), ((), ())), preferred_element_type=F32
            )
        return carry

    lax.fori_loop(0, PARTS, first_dot, 0)
    load_a(1).start()
    load_g(2).start()
    load_x(0).start()
    pl.semaphore_wait(barrier, 4)

    def aslot(q):
        return jnp.where(q == whole, ACC, q % ACC)

    def row0(c, k):
        return pl.multiple_of(c * half + k * band, 16)

    def lane0(l):
        return pl.multiple_of(l * LANE, LANE)

    def piece(q, c, k, l, r0_=0, n=None):
        return out.at[q, pl.ds(row0(c, k) + r0_, band if n is None else n), pl.ds(lane0(l), LANE)]

    def remote(s, q, c, d):
        first, second = c, 1 - c
        p1, p2 = pos[first], pos[second]
        axis = first if s in (0, 1, 6, 7) else second
        w, r = q % SENT, q % RING
        if s == 0:
            src, dst = s0.at[c, d, w], r0.at[c, d, r]
        elif s == 1:
            src, dst = s1.at[c, d, w], r1.at[c, d, r]
        elif s == 2:
            src, dst = (s2p.at[c, w], r2p.at[c, r]) if d == 0 else (s2m.at[c, w], r2m.at[c, r])
        elif s == 3:
            src, dst = s3.at[c, d, w], r3.at[c, d, r]
        elif s == 4:
            src = dst = piece(q, c, p1, p2)
        elif s == 5:
            if d == 0:
                src = dst = piece(q, c, p1, ring(p2 - 1), 0, down)
            else:
                src = dst = piece(q, c, p1, ring(p2 + 1), down, up)
        elif s == 6:
            src = dst = out.at[q, pl.ds(row0(c, p1), band), :]
        else:
            k = ring(p1 - 1) if d == 0 else ring(p1 + 1)
            src = dst = out.at[q, pl.ds(row0(c, k), band), pl.ds(d * hc, hc)]
        return pltpu.make_async_remote_copy(
            src_ref=src, dst_ref=dst,
            send_sem=send_sem.at[s, c, d, w], recv_sem=recv_sem.at[s, c, d, r],
            device_id=near[axis][d], device_id_type=MESH,
        )

    def reuse(s, q):
        @pl.when(q >= SENT)
        def _():
            for d in range(2):
                for c in range(2):
                    remote(s, q, c, d).wait_send()

    def step0(q):
        slot = aslot(q)
        reuse(0, q)
        for d in range(2):
            for c in range(2):
                k = ring(pos[c] + 2)
                s0[c, d, q % SENT] = acc[slot, pl.ds(row0(c, k), band), pl.ds(d * hc, hc)].astype(BF)
                remote(0, q, c, d).start()

    def step1(q):
        slot = aslot(q)
        reuse(1, q)
        for d in range(2):
            for c in range(2):
                remote(0, q, c, d).wait_recv()
                k = ring(pos[c] + (1 if d == 0 else -1))
                r = pl.ds(row0(c, k), band)
                w = q % SENT
                mine, other = pl.ds(d * hc, hc), pl.ds((1 - d) * hc, hc)
                s1[c, d, w, :, mine] = (acc[slot, r, mine] + r0[c, d, q % RING].astype(F32)).astype(BF)
                s1[c, d, w, :, other] = acc[slot, r, other].astype(BF)
                remote(1, q, c, d).start()

    def summed(q, c, l, r0_, n):
        z, lanes = q % RING, pl.ds(lane0(l), LANE)
        v = acc[aslot(q), pl.ds(row0(c, pos[c]) + r0_, n), lanes]
        rs = pl.ds(r0_, n)
        return v + r1[c, 0, z, rs, lanes].astype(F32) + r1[c, 1, z, rs, lanes].astype(F32)

    def step2(q):
        reuse(2, q)
        for c in range(2):
            for d in range(2):
                remote(1, q, c, d).wait_recv()
            l = ring(pos[1 - c] + 2)
            w = q % SENT
            for d in range(2):
                if d == 0:
                    s2p[c, w] = summed(q, c, l, 0, up).astype(BF)
                else:
                    s2m[c, w] = summed(q, c, l, up, down).astype(BF)
                remote(2, q, c, d).start()

    def step3(q):
        reuse(3, q)
        for d in range(2):
            for c in range(2):
                remote(2, q, c, d).wait_recv()
                l = ring(pos[1 - c] + (1 if d == 0 else -1))
                w, z = q % SENT, q % RING
                top, low = summed(q, c, l, 0, up), summed(q, c, l, up, down)
                if d == 0:
                    top = top + r2p[c, z].astype(F32)
                else:
                    low = low + r2m[c, z].astype(F32)
                s3[c, d, w, pl.ds(0, up)] = top.astype(BF)
                s3[c, d, w, pl.ds(up, down)] = low.astype(BF)
                remote(3, q, c, d).start()

    def step4(q):
        reuse(4, q)
        z = q % RING
        for c in range(2):
            for d in range(2):
                remote(3, q, c, d).wait_recv()
            v = summed(q, c, pos[1 - c], 0, band) + r3[c, 0, z].astype(F32) + r3[c, 1, z].astype(F32)
            out[q, pl.ds(row0(c, pos[c]), band), pl.ds(lane0(pos[1 - c]), LANE)] = v.astype(BF)
            for d in range(2):
                remote(4, q, c, d).start()

        @pl.when(q + RING < total)
        def _():
            for axis in range(2):
                for d in range(2):
                    pl.semaphore_signal(
                        credit.at[axis, d], inc=1, device_id=near[axis][d], device_id_type=MESH
                    )

    def arrived(s, q, c, d):
        first, second = c, 1 - c
        p1, p2 = pos[first], pos[second]
        back = -1 if d == 0 else 1
        if s == 4:
            dst = piece(q, c, p1, ring(p2 + back))
        elif s == 5:
            dst = piece(q, c, p1, ring(p2 + 2), 0, down) if d == 0 else piece(q, c, p1, ring(p2 + 2), down, up)
        elif s == 6:
            dst = out.at[q, pl.ds(row0(c, ring(p1 + back)), band), :]
        else:
            dst = out.at[q, pl.ds(row0(c, ring(p1 + 2)), band), pl.ds(d * hc, hc)]
        axis = second if s in (4, 5) else first
        pltpu.make_async_remote_copy(
            src_ref=dst, dst_ref=dst,
            send_sem=send_sem.at[s, c, d, q % SENT], recv_sem=recv_sem.at[s, c, d, q % RING],
            device_id=near[axis][d], device_id_type=MESH,
        ).wait_recv()

    def step5(q):
        reuse(5, q)
        for d in range(2):
            for c in range(2):
                arrived(4, q, c, d)
                remote(5, q, c, d).start()

    def step6(q):
        reuse(6, q)
        for c in range(2):
            for d in range(2):
                arrived(5, q, c, d)
            for d in range(2):
                remote(6, q, c, d).start()

    def step7(q):
        reuse(7, q)
        for d in range(2):
            for c in range(2):
                arrived(6, q, c, d)
                remote(7, q, c, d).start()

    def step8(q):
        for d in range(2):
            for c in range(2):
                arrived(7, q, c, d)

    def dot(n, w):
        return lax.dot_general(abuf[n % 2], w, (((0,), (0,)), ((), ())), preferred_element_type=F32)

    def stage(t, s, f):
        @pl.when((t >= s) & (t < total + s))
        def _():
            f(t - s)

    steps = (step0, step1, step2, step3, step4, step5, step6, step7, step8)

    def turn(t, carry):
        u = t + 1
        n, c = u // per, u % per

        @pl.when((t >= RING) & (t < total))
        def _():
            for axis in range(2):
                for d in range(2):
                    pl.semaphore_wait(credit.at[axis, d], 1)

        def product(h, first, last):
            @pl.when(u < whole)
            def _():
                if first:
                    @pl.when(c == 0)
                    def _():
                        load_a(n).wait()

                    load_g(u).wait()
                lanes = pl.ds(h * hc, hc)
                acc[u % ACC, :, lanes] = dot(n, gbuf[u % 2, :, lanes])
                if last:
                    @pl.when(u + 2 < whole)
                    def _():
                        load_g(u + 2).start()

        def odd():
            @pl.when((c == 0) & (u <= whole))
            def _():
                load_x(n - 1).wait()
                acc[ACC, :, pl.ds(lane0(n - 1), LANE)] = dot(n - 1, xbuf[...])

                @pl.when(n < mats)
                def _():
                    load_x(n).start()

                @pl.when(n + 1 < mats)
                def _():
                    load_a(n + 1).start()

        done = 0
        for item in ORDER:
            if item == "D":
                product(done, done == 0, done == 1)
                done += 1
            elif item == "X":
                odd()
            else:
                stage(t, LAG[item], steps[item])
        return carry

    lax.fori_loop(0, total + LAG[8], turn, 0)

    for s in range(8):
        for c in range(2):
            for d in range(2):
                for k in range(SENT):
                    remote(s, total - SENT + k, c, d).wait_send()


def write(per, sums, out, sem):
    mats = out.shape[0]
    chunk = sums.shape[2]
    copies = []
    for n in range(mats):
        for c in range(per):
            copies.append((sums.at[n * per + c], out.at[n, :, pl.ds(c * chunk, chunk)]))
        copies.append((sums.at[mats * per, :, pl.ds(n * LANE, LANE)], out.at[n, :, pl.ds(per * chunk, LANE)]))
    copies = [pltpu.make_async_copy(s, d, sem.at[i]) for i, (s, d) in enumerate(copies)]
    for copy in copies:
        copy.start()
    for copy in copies:
        copy.wait()


def solution(mesh):
    side = math.isqrt(mesh.shape["dp"])

    def step(a, g):
        a, g = a[0], g[0]
        mats, tokens, rows = a.shape
        cols = g.shape[2]
        chunk = side * LANE
        per = cols // chunk
        total = mats * per + 1
        band, hc = rows // 2 // side, chunk // 2
        up = (band // 2 + 15) // 16 * 16
        down = band - up
        dma = pltpu.SemaphoreType.DMA
        sums = pl.pallas_call(
            functools.partial(kernel, side),
            out_shape=pltpu.VMEM((total, rows, chunk), BF),
            in_specs=[pl.BlockSpec(memory_space=pl.ANY)] * 2,
            out_specs=pl.BlockSpec(memory_space=pltpu.VMEM),
            scratch_shapes=[
                pltpu.VMEM((2, tokens, rows), BF),
                pltpu.VMEM((2, tokens, chunk), BF),
                pltpu.VMEM((tokens, LANE), BF),
                pltpu.VMEM((ACC + 1, rows, chunk), F32),
                pltpu.VMEM((2, 2, SENT, band, hc), BF),
                pltpu.VMEM((2, 2, SENT, band, chunk), BF),
                pltpu.VMEM((2, SENT, up, LANE), BF),
                pltpu.VMEM((2, SENT, down, LANE), BF),
                pltpu.VMEM((2, 2, SENT, band, LANE), BF),
                pltpu.VMEM((2, 2, RING, band, hc), BF),
                pltpu.VMEM((2, 2, RING, band, chunk), BF),
                pltpu.VMEM((2, RING, up, LANE), BF),
                pltpu.VMEM((2, RING, down, LANE), BF),
                pltpu.VMEM((2, 2, RING, band, LANE), BF),
                dma((2,)),
                dma((2,)),
                dma(()),
                dma((2, PARTS)),
                dma((8, 2, 2, SENT)),
                dma((8, 2, 2, RING)),
                pltpu.SemaphoreType.REGULAR((2, 2)),
            ],
            compiler_params=pltpu.CompilerParams(
                collective_id=0, has_side_effects=True, vmem_limit_bytes=45 * 2**20
            ),
        )(a, g)
        return pl.pallas_call(
            functools.partial(write, per),
            out_shape=jax.ShapeDtypeStruct((mats, rows, cols), BF),
            in_specs=[pl.BlockSpec(memory_space=pltpu.VMEM)],
            out_specs=pl.BlockSpec(memory_space=pl.ANY),
            scratch_shapes=[dma((mats * (per + 1),))],
            compiler_params=pltpu.CompilerParams(vmem_limit_bytes=2**20),
        )(sums)

    return jax.shard_map(
        step,
        mesh=mesh,
        in_specs=(P(("rep", "dp")), P(("rep", "dp"))),
        out_specs=P("rep"),
        check_vma=False,
    )
```
